32 devices in a mesh: img: 2 (over x), neu: 16 (over z, y, core).
Axes of the slice: x: 2, y: 2, z: 4, core: 2. Of those that a mesh axis runs over, the one named last changes fastest.
Arguments:
- image_values: bfloat16 [4096, 1024], P('neu', 'img'), may hold values from 0.25 to 16
- image_mask: int32 [4096, 1024], P('neu', 'img'), may hold values 0 or 1
- weights: bfloat16 [3, 4096, 4, 8], P(None, 'neu'), may hold values from -0.25 to 0.34960938
- block_index: int32 [3, 128, 4], P(None, 'neu'), may hold values from 0 to 511, as said below
Outputs:
- activations: bfloat16 [4096, 1024], P('neu', 'img')
- row_sums: float32 [1024], P(('img', 'neu'))
The draws below stay inside these ranges and needn't reach their ends.
Inputs may be any that keep to these rules, and one draw needn't show every extreme that they name: Split the 512 input blocks into 16 runs of consecutive blocks, and the 128 output blocks likewise; if output block b lies in run s, block_index[l, b, k] lies in run (s + k * 4 + l) mod 16.
All inputs are finite; a program needn't handle non-finite values. No bound on the sum of `image_mask` on one device may be relied on, other than what follows from the above.
Results may differ from the reference program's by a relative error of at most 0.0035.
Values may be sent and summed in bfloat16 or wider, within the bound.
A program may use at most 64 MiB of HBM per device.

```python
import math
import jax
import jax.numpy as jnp

NEU = 4096
LAYERS = 3
KB = 4
IB = 8
OB = 32
IMAGES = 1024
NOB = 128
N_NEU = 16


def draw_block_index(key, part):
    per_run = NEU // IB // N_NEU
    outs_per_run = NOB // N_NEU
    owner = jnp.arange(NOB, dtype=jnp.int32) // outs_per_run
    layer_ids = jnp.arange(LAYERS, dtype=jnp.int32)
    slot_ids = jnp.arange(KB, dtype=jnp.int32)
    source = (owner[None, :, None] + slot_ids[None, None, :] * (N_NEU // KB) + layer_ids[:, None, None]) % N_NEU
    inner = jax.random.randint(jax.random.fold_in(key, 7), (LAYERS, NOB, KB), 0, per_run, dtype=jnp.int32)
    return (source * per_run + inner).astype(jnp.int32)


def place_ends(values, stream_key, low, high):
    extent = values.shape
    index_at = [jax.random.randint(jax.random.fold_in(stream_key, axis), (), 0, extent[axis]) for axis in range(len(extent))]
    values = values.at[tuple(index_at)].set(low)
    longest = extent.index(max(extent))
    index_at[longest] = (index_at[longest] + 1) % extent[longest]
    return values.at[tuple(index_at)].set(high)


def block_scale(stream_key, extent, pieces, least, high):
    factor_of, own = 1.0, jax.random.fold_in(stream_key, 6)
    for dim, blocks in pieces:
        draws = jnp.exp(jax.random.uniform(jax.random.fold_in(own, dim), (blocks,), jnp.float32, least / len(pieces), high / len(pieces)))
        factor_of = factor_of * jnp.repeat(draws, extent[dim] // blocks).reshape([-1 if axis == dim else 1 for axis in range(len(extent))])
    return factor_of


def setup_inputs(seed: int = 0) -> dict:
    splits = jax.random.split(jax.random.key(seed), 5)
    return {
        "image_values": jnp.clip(jnp.exp(math.log(16.0) - 4.158883 * jax.random.uniform(splits[0], (NEU, IMAGES), jnp.float32) ** block_scale(splits[0], (NEU, IMAGES), ((0, 16), (1, 2)), -0.2, 0.2)), 0.25, 16.0).astype(jnp.bfloat16),
        "image_mask": place_ends((jax.random.randint(splits[1], (NEU, IMAGES), 0, 2) < 1).astype(jnp.int32), jax.random.fold_in(splits[1], 1), 0, 1),
        "weights": jnp.clip(-0.25 + 0.5996094 * jax.random.uniform(splits[2], (LAYERS, NEU, KB, IB), jnp.float32) ** block_scale(splits[2], (LAYERS, NEU, KB, IB), ((1, 16),), -0.2, 0.2), -0.25, 0.34960938).astype(jnp.bfloat16),
        "block_index": draw_block_index(jax.random.fold_in(splits[4], 71), 0),
    }


bias_value = 0.35
ceiling = 32.0


def advance(activity, layer_weights, layer_blocks):
    offsets = jnp.arange(IB, dtype=jnp.int32)
    rows_wanted = (layer_blocks.astype(jnp.int32)[:, :, None] * IB + offsets[None, None, :]).reshape(-1)
    picked = jnp.take(activity, rows_wanted, axis=0).reshape(layer_blocks.shape[0], KB * IB, -1).astype(jnp.float32)
    weights_full = layer_weights.reshape(layer_blocks.shape[0], OB, KB * IB).astype(jnp.float32)
    summed = jnp.einsum("dom,dmr->dor", weights_full, picked)
    clamped = jnp.minimum(jnp.maximum(summed - bias_value, 0.0), ceiling)
    return clamped.astype(jnp.bfloat16).reshape(NEU, -1)


def reference(image_values, image_mask, weights, block_index):
    activity = image_values * image_mask.astype(jnp.bfloat16)
    for layer_number in range(LAYERS):
        activity = advance(activity, weights[layer_number], block_index[layer_number])
    totals = jnp.sum(activity.astype(jnp.float32), axis=0)
    return activity, totals
```

```python
import functools

import jax
import jax.numpy as jnp
from jax import lax
from jax.experimental import pallas as pl
from jax.experimental.pallas import tpu as pltpu
from jax.sharding import PartitionSpec as P

KB = 4
IB = 8
OB = 32

bias_value = 0.35
ceiling = 32.0


def quotient(x, n):
    return x >> (n.bit_length() - 1) if n & (n - 1) == 0 else lax.div(x, jnp.int32(n))


def remainder(x, n):
    return x & (n - 1) if n & (n - 1) == 0 else lax.rem(x, jnp.int32(n))


def by_position(q, values):
    return (sum(v << (2 * i) for i, v in enumerate(values)) >> (2 * q)) & 3


def kernel(
    geometry, val_hbm, mask_hbm, wt_hbm, idx_hbm, out_ref, rs_ref,
    val, mask, w_src, i_src, i_out, y0, xin, ya, yb, wt, wd, idx_v, idx_s, tiles, part, parts,
    load_sem, own_sem, w_send, w_recv, f_recv, i_send, i_recv, s_sem, in_send, in_recv, o_send, o_recv,
    r_send, r_recv, here_sem,
):
    classes, pairs, layers, rows, blocks, lanes = geometry
    group = KB
    last = layers - 1
    shift = [l * (l + 1) // 2 % classes for l in range(layers)]
    me = lax.axis_index("neu")
    q, c = me // classes, me % classes
    run_blocks = rows // IB

    middle = (q == 1) | (q == 2)
    other = by_position(q, [3, 2, 1, 0])
    near = by_position(q, [1, 0, 3, 2])
    far = by_position(q, [2, 3, 0, 1])
    order = [
        by_position(q, [3, 3, 0, 0]), by_position(q, [0, 2, 1, 3]),
        by_position(q, [2, 0, 3, 1]), by_position(q, [1, 1, 2, 2]),
    ]

    def to(z, dc):
        return {"neu": z * classes + (c + dc) % classes}

    def remote(src, dst, send, recv, device_id):
        x = pltpu.make_async_remote_copy(
            src_ref=src, dst_ref=dst, send_sem=send, recv_sem=recv,
            device_id=device_id, device_id_type=pl.DeviceIdType.MESH,
        )
        x.start()

    def wait(ref, sem):
        pltpu.make_async_copy(ref, ref, sem).wait()

    own = [
        pltpu.make_async_copy(wt_hbm, w_src, own_sem.at[0]),
        pltpu.make_async_copy(idx_hbm, i_src, own_sem.at[1]),
    ]
    for a in own:
        a.start()
    for p, t in enumerate(order):
        cols = pl.ds(pl.multiple_of(t * lanes, lanes), lanes)
        pltpu.make_async_copy(val_hbm.at[:, cols], val.at[p], load_sem.at[0]).start()
        pltpu.make_async_copy(mask_hbm.at[:, cols], mask.at[p], load_sem.at[1]).start()

    barrier = pltpu.get_barrier_semaphore()
    x_me = lax.axis_index("img")
    half = x_me % 2
    twin = {"img": x_me + 1 - 2 * half}
    share_rows = KB * IB // 2
    w_rows = pl.ds(pl.multiple_of(half * share_rows, share_rows), share_rows) if pairs else pl.ds(0, KB * IB)

    @pl.when(middle)
    def _():
        greet = [to(z, -s) for s in sorted(set(shift)) for z in (far, other)]
        greet += [to(near, dc) for dc in range(classes)]
        greet += [to(q, dc) for dc in range(1, classes)]
        if pairs:
            greet.append(twin)
        for device in greet:
            pl.semaphore_signal(barrier, inc=1, device_id=device, device_id_type=pl.DeviceIdType.MESH)

    def masked(p):
        y0[p] = (val[p].astype(jnp.float32) * mask[p].astype(jnp.float32)).astype(jnp.bfloat16)

    for a in own:
        a.wait()
    b = i_src[...]
    i_out[...] = quotient(b, run_blocks * classes) * run_blocks + remainder(b, run_blocks)

    def send_weights(l, z):
        n = q * layers + l
        remote(i_out.at[l], idx_v.at[n], i_send, i_recv, to(z, shift[l]))
        remote(w_src.at[l, w_rows], wt.at[n, w_rows], w_send, w_recv.at[q], to(z, shift[l]))

    def send_input(p, chunk, z):
        remote(y0.at[p], xin.at[chunk, q], in_send, in_recv.at[chunk], to(z, 0))

    unknown = [dc for dc in range(classes) if dc not in shift]

    def own_share(total):
        row = jnp.sum(total, axis=0, keepdims=True)
        share = lanes // classes
        mine = jnp.zeros((1, share), jnp.float32)
        for j in range(classes):
            mine = jnp.where(c == j, row[:, j * share:(j + 1) * share], mine)
        rs_ref[...] = mine

    @pl.when(jnp.logical_not(middle))
    def _():
        pl.semaphore_wait(barrier, classes + len(set(shift)))
        for z in (far, near):
            for l in range(layers):
                send_weights(l, z)
        for dc in unknown:
            pl.semaphore_signal(here_sem, inc=1, device_id=to(near, dc), device_id_type=pl.DeviceIdType.MESH)
        wait(val, load_sem.at[0])
        wait(mask, load_sem.at[1])
        for p in range(group):
            masked(p)
            send_input(p, p // 2, (far, near)[p % 2])
        sent = wt.at[pl.ds(0, 2 * layers), w_rows]
        wait(sent, w_send)
        wait(idx_v.at[pl.ds(0, 2 * layers)], i_send)
        wait(y0, in_send)
        wait(parts.at[pl.ds(0, classes)], r_recv.at[0])
        own_share(sum(parts[dc] for dc in range(classes)))
        wait(out_ref, o_recv)

    @pl.when(middle)
    def _():
        pl.semaphore_wait(barrier, classes - 1 + len(set(shift)) + (1 if pairs else 0))
        for l in range(layers):
            send_weights(l, other)
        for l in range(layers):
            if shift[l]:
                send_weights(l, q)
            else:
                wt[q * layers + l] = w_src[l]
                idx_v[q * layers + l] = i_out[l]
        wait(val, load_sem.at[0])
        wait(mask, load_sem.at[1])
        masked(0)
        send_input(0, 0, other)
        masked(1)
        send_input(1, 1, other)
        masked(2)
        masked(3)

        local = sum(1 for s in shift if s == 0)
        per = min(4, blocks)
        width = per * OB
        m_of = lax.broadcasted_iota(jnp.int32, (width, width), 0) // (KB * IB)
        n_of = lax.broadcasted_iota(jnp.int32, (width, width), 1) // OB

        def pieces_of(z):
            first = local if z is q else 0
            return wt.at[pl.ds(z * layers + first, layers - first), w_rows]

        def pass_on(z):
            here = pieces_of(z)
            wait(here, w_recv.at[z])
            if pairs:
                remote(here, here, w_send, f_recv.at[z], twin)

        def prepare(z):
            if pairs:
                wait(pieces_of(z), f_recv.at[z])
            for l in range(layers):
                for g in range(blocks // per):
                    w = wt[z * layers + l, :, g * width:(g + 1) * width].astype(jnp.float32)
                    wide = jnp.where(m_of == n_of, jnp.concatenate([w] * per, axis=0), 0.0)
                    wd[l, z, g] = wide.T.astype(jnp.bfloat16)

        def advance(l, src, t):
            out = []
            for g in range(blocks // per):
                pieces = [src[idx_s[t * layers + l, k, j]] for j in range(g * per, (g + 1) * per) for k in range(KB)]
                picked = jnp.concatenate(pieces, axis=0).astype(jnp.bfloat16)
                summed = jnp.dot(wd[l, t, g], picked, preferred_element_type=jnp.float32)
                clamped = jnp.minimum(jnp.maximum(summed - bias_value, 0.0), ceiling)
                out.append(clamped.astype(jnp.bfloat16))
            return out

        for z in (q, other, near, far):
            pass_on(z)
        wait(idx_v.at[pl.ds(0, group * layers - local)], i_recv)
        index_copy = pltpu.make_async_copy(idx_v, idx_s, s_sem)
        index_copy.start()
        prepare(q)
        prepare(other)
        prepare(near)
        prepare(far)
        index_copy.wait()
        pl.semaphore_wait(here_sem, len(unknown))

        for chunk in range(2):
            own_rows = y0[2 + chunk].astype(jnp.float32)
            ya[pl.ds(q * run_blocks, run_blocks)] = own_rows.reshape(run_blocks, IB, lanes)
            wait(xin.at[chunk, pl.ds(0, group - 1)], in_recv.at[chunk])
            for z in (other, near, far):
                ya[pl.ds(z * run_blocks, run_blocks)] = xin[chunk, z].astype(jnp.float32).reshape(run_blocks, IB, lanes)

            src, dst = ya, yb
            for l in range(last):
                for t in range(group):
                    for g, y in enumerate(advance(l, src, t)):
                        first = t * run_blocks + g * width // IB
                        dst[first:first + width // IB] = y.astype(jnp.float32).reshape(width // IB, IB, lanes)
                src, dst = dst, src

            tile = near if chunk == 0 else q
            cols = pl.ds(pl.multiple_of(tile * lanes, lanes), lanes)
            targets = (far, near, other, q)
            total = jnp.zeros((8, lanes), jnp.float32)

            def send_tile(d):
                remote(tiles.at[chunk, d], out_ref.at[:, cols], o_send, o_recv, to(targets[d], -shift[last]))

            ready = None
            for d in range(group + 1):
                fresh = advance(last, src, targets[d]) if d < group else None
                if ready is not None:
                    for g, y in enumerate(ready):
                        tiles[chunk, d - 1, g * width:(g + 1) * width, :] = y
                        total = total + jnp.sum(y.astype(jnp.float32).reshape(width // 8, 8, lanes), axis=0)
                    if chunk == 0:
                        send_tile(d - 1)
                ready = fresh
            part[chunk] = total
            for dc in range(chunk, classes):
                where = to(q, dc) if chunk else to(near, dc)
                remote(part.at[chunk], parts.at[chunk * classes + dc], r_send, r_recv.at[chunk], where)
            if chunk:
                for d in range(group):
                    send_tile(d)

        wait(parts.at[pl.ds(classes + 1, classes - 1)], r_recv.at[1])
        own_share(part[1] + sum(parts[classes + dc] for dc in range(1, classes)))
        if pairs:
            wait(wt.at[pl.ds(0, 3 * layers - local)], w_send)
        else:
            wait(wt.at[pl.ds(0, 2 * layers - local)], w_send)
        wait(idx_v.at[pl.ds(0, 2 * layers - local)], i_send)
        wait(y0.at[pl.ds(0, 2)], in_send)
        wait(tiles, o_send)
        wait(parts.at[pl.ds(0, 2 * classes - 1)], r_send)
        wait(out_ref, o_recv)


def store(out_ref, rs_ref, out_hbm, rs_hbm, sems):
    a = pltpu.make_async_copy(out_ref, out_hbm, sems.at[0])
    b = pltpu.make_async_copy(rs_ref, rs_hbm, sems.at[1])
    a.start()
    b.start()
    a.wait()
    b.wait()


def on_device(classes, pairs, image_values, image_mask, weights, block_index):
    layers, rows = weights.shape[:2]
    blocks = block_index.shape[1]
    columns = image_values.shape[1]
    group = KB
    lanes = columns // group
    wt = jnp.transpose(weights, (0, 2, 3, 1)).reshape(layers, KB * IB, rows)
    idx = jnp.transpose(block_index, (0, 2, 1))
    per = min(4, blocks)
    bf16, f32, i32 = jnp.bfloat16, jnp.float32, jnp.int32
    V, S = pltpu.VMEM, pltpu.SMEM
    dma = pltpu.SemaphoreType.DMA
    any_spec = pl.BlockSpec(memory_space=pl.ANY)
    operands = [pltpu.with_memory_space_constraint(v, pltpu.HBM) for v in (image_values, image_mask, wt, idx)]
    out, sums = pl.pallas_call(
        functools.partial(kernel, (classes, pairs, layers, rows, blocks, lanes)),
        out_shape=(
            jax.ShapeDtypeStruct((rows, columns), bf16),
            jax.ShapeDtypeStruct((1, lanes // classes), f32),
        ),
        in_specs=[any_spec] * 4,
        out_specs=(pl.BlockSpec(memory_space=pltpu.VMEM), pl.BlockSpec(memory_space=pltpu.VMEM)),
        scratch_shapes=[
            V((group, rows, lanes), bf16),
            V((group, rows, lanes), i32),
            V((layers, KB * IB, rows), bf16),
            V((layers, KB, blocks), i32),
            V((layers, KB, blocks), i32),
            V((group, rows, lanes), bf16),
            V((2, group, rows, lanes), bf16),
            V((group * rows // IB, IB, lanes), f32),
            V((group * rows // IB, IB, lanes), f32),
            V((group * layers, KB * IB, rows), bf16),
            V((layers, group, blocks // per, per * OB, per * KB * IB), bf16),
            V((group * layers, KB, blocks), i32),
            S((group * layers, KB, blocks), i32),
            V((2, group, rows, lanes), bf16),
            V((2, 8, lanes), f32),
            V((2 * classes, 8, lanes), f32),
            dma((2,)), dma((2,)),
            dma(()), dma((group,)), dma((group,)),
            dma(()), dma(()), dma(()),
            dma(()), dma((2,)),
            dma(()), dma(()),
            dma(()), dma((2,)), pltpu.SemaphoreType.REGULAR,
        ],
        compiler_params=pltpu.CompilerParams(collective_id=0, has_side_effects=True, vmem_limit_bytes=16 * 1024 * 1024),
    )(*operands)
    vmem_spec = pl.BlockSpec(memory_space=pltpu.VMEM)
    out, sums = pl.pallas_call(
        store,
        out_shape=(jax.ShapeDtypeStruct(out.shape, out.dtype), jax.ShapeDtypeStruct(sums.shape, sums.dtype)),
        in_specs=[vmem_spec] * 2,
        out_specs=(any_spec, any_spec),
        scratch_shapes=[dma((2,))],
    )(*(pltpu.with_memory_space_constraint(v, pltpu.VMEM) for v in (out, sums)))
    return out, sums.reshape(-1)


def solution(mesh):
    classes = mesh.shape["neu"] // KB
    in_specs = (P("neu", "img"), P("neu", "img"), P(None, "neu", None, None), P(None, "neu", None))
    out_specs = (P("neu", "img"), P(("img", "neu")))
    return jax.shard_map(
        functools.partial(on_device, classes, mesh.shape["img"] % 2 == 0), mesh=mesh, in_specs=in_specs,
        out_specs=out_specs, check_vma=False,
    )
```

```python
import functools

import jax
import jax.numpy as jnp
from jax import lax
from jax.experimental import pallas as pl
from jax.experimental.pallas import tpu as pltpu
from jax.sharding import PartitionSpec as P

KB = 4
IB = 8
OB = 32

bias_value = 0.35
ceiling = 32.0


def quotient(x, n):
    return x >> (n.bit_length() - 1) if n & (n - 1) == 0 else lax.div(x, jnp.int32(n))


def remainder(x, n):
    return x & (n - 1) if n & (n - 1) == 0 else lax.rem(x, jnp.int32(n))


def by_position(q, values):
    return (sum(v << (2 * i) for i, v in enumerate(values)) >> (2 * q)) & 3


def kernel(
    geometry, val_hbm, mask_hbm, wt_hbm, idx_hbm, out_ref, rs_ref,
    val, mask, w_src, i_src, i_out, y0, xin, ya, yb, wt, wd, idx_v, idx_s, tiles, part, parts,
    load_sem, own_sem, w_send, w_recv, n_send, f_recv, i_send, i_recv, s_sem, in_send, in_recv, o_send, o_recv,
    r_send, r_recv, here_sem,
):
    classes, pairs, layers, rows, blocks, lanes = geometry
    group = KB
    last = layers - 1
    shift = [l * (l + 1) // 2 % classes for l in range(layers)]
    me = lax.axis_index("neu")
    q, c = me // classes, me % classes
    run_blocks = rows // IB

    middle = (q == 1) | (q == 2)
    other = by_position(q, [3, 2, 1, 0])
    near = by_position(q, [1, 0, 3, 2])
    far = by_position(q, [2, 3, 0, 1])
    order = [
        by_position(q, [3, 3, 0, 0]), by_position(q, [0, 2, 1, 3]),
        by_position(q, [2, 0, 3, 1]), by_position(q, [1, 1, 2, 2]),
    ]

    def to(z, dc):
        return {"neu": z * classes + (c + dc) % classes}

    def remote(src, dst, send, recv, device_id):
        x = pltpu.make_async_remote_copy(
            src_ref=src, dst_ref=dst, send_sem=send, recv_sem=recv,
            device_id=device_id, device_id_type=pl.DeviceIdType.MESH,
        )
        x.start()

    def wait(ref, sem):
        pltpu.make_async_copy(ref, ref, sem).wait()

    own = [
        pltpu.make_async_copy(wt_hbm, w_src, own_sem.at[0]),
        pltpu.make_async_copy(idx_hbm, i_src, own_sem.at[1]),
    ]
    for a in own:
        a.start()
    for p, t in enumerate(order):
        cols = pl.ds(pl.multiple_of(t * lanes, lanes), lanes)
        pltpu.make_async_copy(val_hbm.at[:, cols], val.at[p], load_sem.at[0]).start()
        pltpu.make_async_copy(mask_hbm.at[:, cols], mask.at[p], load_sem.at[1]).start()

    barrier = pltpu.get_barrier_semaphore()
    x_me = lax.axis_index("img")
    half = x_me % 2
    twin = {"img": x_me + 1 - 2 * half}
    share_rows = KB * IB // 2
    w_rows = pl.ds(pl.multiple_of(half * share_rows, share_rows), share_rows) if pairs else pl.ds(0, KB * IB)

    @pl.when(middle)
    def _():
        greet = [to(z, -s) for s in sorted(set(shift)) for z in (far, other)]
        greet += [to(near, dc) for dc in range(classes)]
        greet += [to(q, dc) for dc in range(1, classes)]
        if pairs:
            greet.append(twin)
        for device in greet:
            pl.semaphore_signal(barrier, inc=1, device_id=device, device_id_type=pl.DeviceIdType.MESH)

    def masked(p):
        y0[p] = (val[p].astype(jnp.float32) * mask[p].astype(jnp.float32)).astype(jnp.bfloat16)

    for a in own:
        a.wait()
    b = i_src[...]
    i_out[...] = quotient(b, run_blocks * classes) * run_blocks + remainder(b, run_blocks)

    def send_weights(l, z):
        n = q * layers + l
        remote(i_out.at[l], idx_v.at[n], i_send, i_recv, to(z, shift[l]))
        if z is q:
            remote(w_src.at[l], wt.at[n], n_send, w_recv.at[q], to(z, shift[l]))
        else:
            remote(w_src.at[l, w_rows], wt.at[n, w_rows], w_send, w_recv.at[q], to(z, shift[l]))

    def send_input(p, chunk, z):
        remote(y0.at[p], xin.at[chunk, q], in_send, in_recv.at[chunk], to(z, 0))

    unknown = [dc for dc in range(classes) if dc not in shift]

    def own_share(total):
        row = total
        share = lanes // classes
        mine = jnp.zeros((1, share), jnp.float32)
        for j in range(classes):
            mine = jnp.where(c == j, row[:, j * share:(j + 1) * share], mine)
        rs_ref[...] = mine

    @pl.when(jnp.logical_not(middle))
    def _():
        pl.semaphore_wait(barrier, classes + len(set(shift)))
        for z in (far, near):
            for l in range(layers):
                send_weights(l, z)
        for dc in unknown:
            pl.semaphore_signal(here_sem, inc=1, device_id=to(near, dc), device_id_type=pl.DeviceIdType.MESH)
        wait(val, load_sem.at[0])
        wait(mask, load_sem.at[1])
        wait(wt.at[pl.ds(0, 2 * layers), w_rows], w_send)
        for p in range(group):
            masked(p)
            send_input(p, p // 2, (far, near)[p % 2])
        wait(idx_v.at[pl.ds(0, 2 * layers)], i_send)
        wait(y0, in_send)
        wait(parts.at[pl.ds(0, classes)], r_recv.at[0])
        own_share(sum(parts[dc] for dc in range(classes)))
        wait(out_ref, o_recv)

    @pl.when(middle)
    def _():
        pl.semaphore_wait(barrier, classes - 1 + len(set(shift)) + (1 if pairs else 0))
        for l in range(layers):
            send_weights(l, other)
        for l in range(layers):
            if shift[l]:
                send_weights(l, q)
            else:
                wt[q * layers + l] = w_src[l]
                idx_v[q * layers + l] = i_out[l]
        wait(val, load_sem.at[0])
        wait(mask, load_sem.at[1])
        wait(wt.at[pl.ds(0, layers), w_rows], w_send)
        masked(0)
        send_input(0, 0, other)
        masked(1)
        send_input(1, 1, other)
        masked(2)
        masked(3)

        local = sum(1 for s in shift if s == 0)
        per = min(4, blocks)
        width = per * OB
        m_of = lax.broadcasted_iota(jnp.int32, (width, width), 0) // (KB * IB)
        n_of = lax.broadcasted_iota(jnp.int32, (width, width), 1) // OB

        def pieces_of(z):
            if z is q:
                return wt.at[pl.ds(z * layers + local, layers - local)]
            return wt.at[pl.ds(z * layers, layers), w_rows]

        def pass_on(z):
            here = pieces_of(z)
            wait(here, w_recv.at[z])
            if pairs and z is not q:
                remote(here, here, w_send, f_recv.at[z], twin)

        def prepare(z):
            if pairs and z is not q:
                wait(pieces_of(z), f_recv.at[z])
            for l in range(layers):
                for g in range(blocks // per):
                    w = wt[z * layers + l, :, g * width:(g + 1) * width].astype(jnp.float32)
                    wide = jnp.where(m_of == n_of, jnp.concatenate([w] * per, axis=0), 0.0)
                    wd[l, z, g] = wide.T.astype(jnp.bfloat16)

        def advance(l, src, t):
            out = []
            for g in range(blocks // per):
                pieces = [src[idx_s[t * layers + l, k, j]] for j in range(g * per, (g + 1) * per) for k in range(KB)]
                picked = jnp.concatenate(pieces, axis=0).astype(jnp.bfloat16)
                summed = jnp.dot(wd[l, t, g], picked, preferred_element_type=jnp.float32)
                clamped = jnp.minimum(jnp.maximum(summed - bias_value, 0.0), ceiling)
                out.append(clamped.astype(jnp.bfloat16))
            return out

        for z,nm in ((q,'own'), (other,'oth'), (near,'nea'), (far,'far')):
            pass_on(z)
        wait(idx_v.at[pl.ds(0, group * layers - local)], i_recv)
        index_copy = pltpu.make_async_copy(idx_v, idx_s, s_sem)
        index_copy.start()
        prepare(q)
        prepare(other)
        prepare(near)
        prepare(far)
        index_copy.wait()
        pl.semaphore_wait(here_sem, len(unknown))

        for chunk in range(2):
            own_rows = y0[2 + chunk].astype(jnp.float32)
            ya[pl.ds(q * run_blocks, run_blocks)] = own_rows.reshape(run_blocks, IB, lanes)
            wait(xin.at[chunk, pl.ds(0, group - 1)], in_recv.at[chunk])
            for z in (other, near, far):
                ya[pl.ds(z * run_blocks, run_blocks)] = xin[chunk, z].astype(jnp.float32).reshape(run_blocks, IB, lanes)

            src, dst = ya, yb
            for l in range(last):
                for t in range(group):
                    for g, y in enumerate(advance(l, src, t)):
                        first = t * run_blocks + g * width // IB
                        dst[first:first + width // IB] = y.astype(jnp.float32).reshape(width // IB, IB, lanes)
                src, dst = dst, src

            tile = near if chunk == 0 else q
            cols = pl.ds(pl.multiple_of(tile * lanes, lanes), lanes)
            targets = (near, far, other, q) if chunk else (near, far, other, q)
            total = jnp.zeros((8, lanes), jnp.float32)

            def send_tile(d):
                remote(tiles.at[chunk, d], out_ref.at[:, cols], o_send, o_recv, to(targets[d], -shift[last]))

            ready = None
            for d in range(group + 1):
                fresh = advance(last, src, targets[d]) if d < group else None
                if ready is not None:
                    for g, y in enumerate(ready):
                        tiles[chunk, d - 1, g * width:(g + 1) * width, :] = y
                        total = total + jnp.sum(y.astype(jnp.float32).reshape(width // 8, 8, lanes), axis=0)
                    if chunk == 0:
                        send_tile(d - 1)
                ready = fresh
            part[chunk] = jnp.sum(total, axis=0, keepdims=True)
            for dc in range(chunk, classes):
                where = to(q, dc) if chunk else to(near, dc)
                remote(part.at[chunk], parts.at[chunk * classes + dc], r_send, r_recv.at[chunk], where)
            if chunk:
                for d in range(group):
                    send_tile(d)

        wait(parts.at[pl.ds(classes + 1, classes - 1)], r_recv.at[1])
        own_share(part[1] + sum(parts[classes + dc] for dc in range(1, classes)))
        if pairs:
            wait(wt.at[pl.ds(0, 3 * layers), w_rows], w_send)
        wait(wt.at[pl.ds(0, layers - local)], n_send)
        wait(idx_v.at[pl.ds(0, 2 * layers - local)], i_send)
        wait(y0.at[pl.ds(0, 2)], in_send)
        wait(tiles, o_send)
        wait(parts.at[pl.ds(0, 2 * classes - 1)], r_send)
        wait(out_ref, o_recv)


def store(out_ref, rs_ref, out_hbm, rs_hbm, sems):
    a = pltpu.make_async_copy(out_ref, out_hbm, sems.at[0])
    b = pltpu.make_async_copy(rs_ref, rs_hbm, sems.at[1])
    a.start()
    b.start()
    a.wait()
    b.wait()


def on_device(classes, pairs, image_values, image_mask, weights, block_index):
    layers, rows = weights.shape[:2]
    blocks = block_index.shape[1]
    columns = image_values.shape[1]
    group = KB
    lanes = columns // group
    wt = jnp.transpose(weights, (0, 2, 3, 1)).reshape(layers, KB * IB, rows)
    idx = jnp.transpose(block_index, (0, 2, 1))
    per = min(4, blocks)
    bf16, f32, i32 = jnp.bfloat16, jnp.float32, jnp.int32
    V, S = pltpu.VMEM, pltpu.SMEM
    dma = pltpu.SemaphoreType.DMA
    any_spec = pl.BlockSpec(memory_space=pl.ANY)
    operands = [pltpu.with_memory_space_constraint(v, pltpu.HBM) for v in (image_values, image_mask, wt, idx)]
    out, sums = pl.pallas_call(
        functools.partial(kernel, (classes, pairs, layers, rows, blocks, lanes)),
        out_shape=(
            jax.ShapeDtypeStruct((rows, columns), bf16),
            jax.ShapeDtypeStruct((1, lanes // classes), f32),
        ),
        in_specs=[any_spec] * 4,
        out_specs=(pl.BlockSpec(memory_space=pltpu.VMEM), pl.BlockSpec(memory_space=pltpu.VMEM)),
        scratch_shapes=[
            V((group, rows, lanes), bf16),
            V((group, rows, lanes), i32),
            V((layers, KB * IB, rows), bf16),
            V((layers, KB, blocks), i32),
            V((layers, KB, blocks), i32),
            V((group, rows, lanes), bf16),
            V((2, group, rows, lanes), bf16),
            V((group * rows // IB, IB, lanes), f32),
            V((group * rows // IB, IB, lanes), f32),
            V((group * layers, KB * IB, rows), bf16),
            V((layers, group, blocks // per, per * OB, per * KB * IB), bf16),
            V((group * layers, KB, blocks), i32),
            S((group * layers, KB, blocks), i32),
            V((2, group, rows, lanes), bf16),
            V((2, 1, lanes), f32),
            V((2 * classes, 1, lanes), f32),
            dma((2,)), dma((2,)),
            dma(()), dma((group,)), dma(()), dma((group,)),
            dma(()), dma(()), dma(()),
            dma(()), dma((2,)),
            dma(()), dma(()),
            dma(()), dma((2,)), pltpu.SemaphoreType.REGULAR,
        ],
        compiler_params=pltpu.CompilerParams(collective_id=0, has_side_effects=True, vmem_limit_bytes=16 * 1024 * 1024),
    )(*operands)
    vmem_spec = pl.BlockSpec(memory_space=pltpu.VMEM)
    out, sums = pl.pallas_call(
        store,
        out_shape=(jax.ShapeDtypeStruct(out.shape, out.dtype), jax.ShapeDtypeStruct(sums.shape, sums.dtype)),
        in_specs=[vmem_spec] * 2,
        out_specs=(any_spec, any_spec),
        scratch_shapes=[dma((2,))],
    )(*(pltpu.with_memory_space_constraint(v, pltpu.VMEM) for v in (out, sums)))
    return out, sums.reshape(-1)


def solution(mesh):
    classes = mesh.shape["neu"] // KB
    in_specs = (P("neu", "img"), P("neu", "img"), P(None, "neu", None, None), P(None, "neu", None))
    out_specs = (P("neu", "img"), P(("img", "neu")))
    return jax.shard_map(
        functools.partial(on_device, classes, mesh.shape["img"] % 2 == 0), mesh=mesh, in_specs=in_specs,
        out_specs=out_specs, check_vma=False,
    )
```

```python
import functools

import jax
import jax.numpy as jnp
from jax import lax
from jax.experimental import pallas as pl
from jax.experimental.pallas import tpu as pltpu
from jax.sharding import PartitionSpec as P

KB = 4
IB = 8
OB = 32

bias_value = 0.35
ceiling = 32.0


def quotient(x, n):
    return x >> (n.bit_length() - 1) if n & (n - 1) == 0 else lax.div(x, jnp.int32(n))


def remainder(x, n):
    return x & (n - 1) if n & (n - 1) == 0 else lax.rem(x, jnp.int32(n))


def by_position(q, values):
    return (sum(v << (2 * i) for i, v in enumerate(values)) >> (2 * q)) & 3


def kernel(
    geometry, val_hbm, mask_hbm, wt_hbm, idx_hbm, out_ref, rs_ref,
    val, mask, w_src, i_src, i_out, y0, xin, ya, yb, wt, wd, idx_v, idx_s, tiles, part, parts,
    load_sem, own_sem, w_send, w_recv, n_send, f_recv, i_send, i_recv, s_sem, in_send, in_recv, o_send, o_recv,
    r_send, r_recv, here_sem,
):
    classes, pairs, layers, rows, blocks, lanes = geometry
    group = KB
    last = layers - 1
    shift = [l * (l + 1) // 2 % classes for l in range(layers)]
    me = lax.axis_index("neu")
    q, c = me // classes, me % classes
    run_blocks = rows // IB

    middle = (q == 1) | (q == 2)
    other = by_position(q, [3, 2, 1, 0])
    near = by_position(q, [1, 0, 3, 2])
    far = by_position(q, [2, 3, 0, 1])
    order = [
        by_position(q, [3, 3, 0, 0]), by_position(q, [0, 2, 1, 3]),
        by_position(q, [2, 0, 3, 1]), by_position(q, [1, 1, 2, 2]),
    ]

    def to(z, dc):
        return {"neu": z * classes + (c + dc) % classes}

    def remote(src, dst, send, recv, device_id):
        x = pltpu.make_async_remote_copy(
            src_ref=src, dst_ref=dst, send_sem=send, recv_sem=recv,
            device_id=device_id, device_id_type=pl.DeviceIdType.MESH,
        )
        x.start()

    def wait(ref, sem):
        pltpu.make_async_copy(ref, ref, sem).wait()

    own = [
        pltpu.make_async_copy(wt_hbm, w_src, own_sem.at[0]),
        pltpu.make_async_copy(idx_hbm, i_src, own_sem.at[1]),
    ]
    for a in own:
        a.start()
    for p, t in enumerate(order):
        cols = pl.ds(pl.multiple_of(t * lanes, lanes), lanes)
        pltpu.make_async_copy(val_hbm.at[:, cols], val.at[p], load_sem.at[0]).start()
        pltpu.make_async_copy(mask_hbm.at[:, cols], mask.at[p], load_sem.at[1]).start()

    barrier = pltpu.get_barrier_semaphore()
    x_me = lax.axis_index("img")
    half = x_me % 2
    twin = {"img": x_me + 1 - 2 * half}
    share_rows = KB * IB // 2
    w_rows = pl.ds(pl.multiple_of(half * share_rows, share_rows), share_rows) if pairs else pl.ds(0, KB * IB)

    @pl.when(middle)
    def _():
        greet = [to(z, -s) for s in sorted(set(shift)) for z in (far, other)]
        greet += [to(near, dc) for dc in range(classes)]
        greet += [to(q, dc) for dc in range(1, classes)]
        if pairs:
            greet.append(twin)
        for device in greet:
            pl.semaphore_signal(barrier, inc=1, device_id=device, device_id_type=pl.DeviceIdType.MESH)

    def masked(p):
        y0[p] = (val[p].astype(jnp.float32) * mask[p].astype(jnp.float32)).astype(jnp.bfloat16)

    for a in own:
        a.wait()
    b = i_src[...]
    i_out[...] = quotient(b, run_blocks * classes) * run_blocks + remainder(b, run_blocks)

    def send_weights(l, z):
        n = q * layers + l
        remote(i_out.at[l], idx_v.at[n], i_send, i_recv, to(z, shift[l]))
        if z is q:
            remote(w_src.at[l], wt.at[n], n_send, w_recv.at[q], to(z, shift[l]))
        else:
            remote(w_src.at[l, w_rows], wt.at[n, w_rows], w_send, w_recv.at[q], to(z, shift[l]))

    def send_input(p, chunk, z):
        remote(y0.at[p], xin.at[chunk, q], in_send, in_recv.at[chunk], to(z, 0))

    unknown = [dc for dc in range(classes) if dc not in shift]

    def own_share(total):
        row = total
        share = lanes // classes
        mine = jnp.zeros((1, share), jnp.float32)
        for j in range(classes):
            mine = jnp.where(c == j, row[:, j * share:(j + 1) * share], mine)
        rs_ref[...] = mine

    @pl.when(jnp.logical_not(middle))
    def _():
        pl.semaphore_wait(barrier, classes + len(set(shift)))
        for z in (far, near):
            for l in range(layers):
                send_weights(l, z)
        for dc in unknown:
            pl.semaphore_signal(here_sem, inc=1, device_id=to(near, dc), device_id_type=pl.DeviceIdType.MESH)
        wait(val, load_sem.at[0])
        wait(mask, load_sem.at[1])
        wait(wt.at[pl.ds(0, 2 * layers), w_rows], w_send)
        for p in range(group):
            masked(p)
            send_input(p, p // 2, (far, near)[p % 2])
        wait(idx_v.at[pl.ds(0, 2 * layers)], i_send)
        wait(y0, in_send)
        wait(parts.at[pl.ds(0, classes)], r_recv.at[0])
        own_share(sum(parts[dc] for dc in range(classes)))
        wait(out_ref, o_recv)

    @pl.when(middle)
    def _():
        pl.semaphore_wait(barrier, classes - 1 + len(set(shift)) + (1 if pairs else 0))
        for l in range(layers):
            send_weights(l, other)
        for l in range(layers):
            if shift[l]:
                send_weights(l, q)
            else:
                wt[q * layers + l] = w_src[l]
                idx_v[q * layers + l] = i_out[l]
        wait(val, load_sem.at[0])
        wait(mask, load_sem.at[1])
        wait(wt.at[pl.ds(0, layers), w_rows], w_send)
        masked(0)
        send_input(0, 0, other)
        masked(1)
        send_input(1, 1, other)
        masked(2)
        masked(3)

        local = sum(1 for s in shift if s == 0)
        per = min(4, blocks)
        width = per * OB
        m_of = lax.broadcasted_iota(jnp.int32, (width, width), 0) // (KB * IB)
        n_of = lax.broadcasted_iota(jnp.int32, (width, width), 1) // OB

        def pieces_of(z):
            if z is q:
                return wt.at[pl.ds(z * layers + local, layers - local)]
            return wt.at[pl.ds(z * layers, layers), w_rows]

        def pass_on(z):
            here = pieces_of(z)
            wait(here, w_recv.at[z])
            if pairs and z is not q:
                remote(here, here, w_send, f_recv.at[z], twin)

        def prepare(z, take=True):
            if pairs and z is not q and take:
                wait(pieces_of(z), f_recv.at[z])
            for l in range(layers):
                for g in range(blocks // per):
                    w = wt[z * layers + l, :, g * width:(g + 1) * width].astype(jnp.float32)
                    wide = jnp.where(m_of == n_of, jnp.concatenate([w] * per, axis=0), 0.0)
                    wd[l, z, g] = wide.T.astype(jnp.bfloat16)

        def advance(l, src, t):
            out = []
            for g in range(blocks // per):
                pieces = [src[idx_s[t * layers + l, k, j]] for j in range(g * per, (g + 1) * per) for k in range(KB)]
                picked = jnp.concatenate(pieces, axis=0).astype(jnp.bfloat16)
                summed = jnp.dot(wd[l, t, g], picked, preferred_element_type=jnp.float32)
                clamped = jnp.minimum(jnp.maximum(summed - bias_value, 0.0), ceiling)
                out.append(clamped.astype(jnp.bfloat16))
            return out

        for z in (other, near, far, q):
            pass_on(z)
        wait(idx_v.at[pl.ds(0, group * layers - local)], i_recv)
        index_copy = pltpu.make_async_copy(idx_v, idx_s, s_sem)
        index_copy.start()
        prepare(q)
        prepare(other)
        prepare(near)
        index_copy.wait()
        if pairs:
            wait(pieces_of(far), f_recv.at[far])
        pl.semaphore_wait(here_sem, len(unknown))

        for chunk in range(2):
            own_rows = y0[2 + chunk].astype(jnp.float32)
            ya[pl.ds(q * run_blocks, run_blocks)] = own_rows.reshape(run_blocks, IB, lanes)
            wait(xin.at[chunk, pl.ds(0, group - 1)], in_recv.at[chunk])
            if chunk == 0:
                prepare(far, False)
            for z in (other, near, far):
                ya[pl.ds(z * run_blocks, run_blocks)] = xin[chunk, z].astype(jnp.float32).reshape(run_blocks, IB, lanes)

            src, dst = ya, yb
            for l in range(last):
                for t in range(group):
                    for g, y in enumerate(advance(l, src, t)):
                        first = t * run_blocks + g * width // IB
                        dst[first:first + width // IB] = y.astype(jnp.float32).reshape(width // IB, IB, lanes)
                src, dst = dst, src

            tile = near if chunk == 0 else q
            cols = pl.ds(pl.multiple_of(tile * lanes, lanes), lanes)
            targets = (near, far, other, q)
            total = jnp.zeros((8, lanes), jnp.float32)

            def send_tile(d):
                remote(tiles.at[chunk, d], out_ref.at[:, cols], o_send, o_recv, to(targets[d], -shift[last]))

            ready = None
            for d in range(group + 1):
                fresh = advance(last, src, targets[d]) if d < group else None
                if ready is not None:
                    for g, y in enumerate(ready):
                        tiles[chunk, d - 1, g * width:(g + 1) * width, :] = y
                        total = total + jnp.sum(y.astype(jnp.float32).reshape(width // 8, 8, lanes), axis=0)
                    if chunk == 0:
                        send_tile(d - 1)
                ready = fresh
            part[chunk] = jnp.sum(total, axis=0, keepdims=True)
            for dc in range(chunk, classes):
                where = to(q, dc) if chunk else to(near, dc)
                remote(part.at[chunk], parts.at[chunk * classes + dc], r_send, r_recv.at[chunk], where)
            if chunk:
                for d in range(group):
                    send_tile(d)

        wait(parts.at[pl.ds(classes + 1, classes - 1)], r_recv.at[1])
        own_share(part[1] + sum(parts[classes + dc] for dc in range(1, classes)))
        if pairs:
            wait(wt.at[pl.ds(0, 3 * layers), w_rows], w_send)
        wait(wt.at[pl.ds(0, layers - local)], n_send)
        wait(idx_v.at[pl.ds(0, 2 * layers - local)], i_send)
        wait(y0.at[pl.ds(0, 2)], in_send)
        wait(tiles, o_send)
        wait(parts.at[pl.ds(0, 2 * classes - 1)], r_send)
        wait(out_ref, o_recv)


def store(out_ref, rs_ref, out_hbm, rs_hbm, sems):
    a = pltpu.make_async_copy(out_ref, out_hbm, sems.at[0])
    step = out_ref.shape[0] // 4
    b = pltpu.make_async_copy(rs_ref, rs_hbm, sems.at[1])
    b.start()
    for n in range(4):
        rows = pl.ds(n * step, step)
        pltpu.make_async_copy(out_ref.at[rows], out_hbm.at[rows], sems.at[0]).start()
    a.wait()
    b.wait()


def on_device(classes, pairs, image_values, image_mask, weights, block_index):
    layers, rows = weights.shape[:2]
    blocks = block_index.shape[1]
    columns = image_values.shape[1]
    group = KB
    lanes = columns // group
    wt = jnp.transpose(weights, (0, 2, 3, 1)).reshape(layers, KB * IB, rows)
    idx = jnp.transpose(block_index, (0, 2, 1))
    per = min(4, blocks)
    bf16, f32, i32 = jnp.bfloat16, jnp.float32, jnp.int32
    V, S = pltpu.VMEM, pltpu.SMEM
    dma = pltpu.SemaphoreType.DMA
    any_spec = pl.BlockSpec(memory_space=pl.ANY)
    operands = [pltpu.with_memory_space_constraint(v, pltpu.HBM) for v in (image_values, image_mask, wt, idx)]
    out, sums = pl.pallas_call(
        functools.partial(kernel, (classes, pairs, layers, rows, blocks, lanes)),
        out_shape=(
            jax.ShapeDtypeStruct((rows, columns), bf16),
            jax.ShapeDtypeStruct((1, lanes // classes), f32),
        ),
        in_specs=[any_spec] * 4,
        out_specs=(pl.BlockSpec(memory_space=pltpu.VMEM), pl.BlockSpec(memory_space=pltpu.VMEM)),
        scratch_shapes=[
            V((group, rows, lanes), bf16),
            V((group, rows, lanes), i32),
            V((layers, KB * IB, rows), bf16),
            V((layers, KB, blocks), i32),
            V((layers, KB, blocks), i32),
            V((group, rows, lanes), bf16),
            V((2, group, rows, lanes), bf16),
            V((group * rows // IB, IB, lanes), f32),
            V((group * rows // IB, IB, lanes), f32),
            V((group * layers, KB * IB, rows), bf16),
            V((layers, group, blocks // per, per * OB, per * KB * IB), bf16),
            V((group * layers, KB, blocks), i32),
            S((group * layers, KB, blocks), i32),
            V((2, group, rows, lanes), bf16),
            V((2, 1, lanes), f32),
            V((2 * classes, 1, lanes), f32),
            dma((2,)), dma((2,)),
            dma(()), dma((group,)), dma(()), dma((group,)),
            dma(()), dma(()), dma(()),
            dma(()), dma((2,)),
            dma(()), dma(()),
            dma(()), dma((2,)), pltpu.SemaphoreType.REGULAR,
        ],
        compiler_params=pltpu.CompilerParams(collective_id=0, has_side_effects=True, vmem_limit_bytes=16 * 1024 * 1024),
    )(*operands)
    vmem_spec = pl.BlockSpec(memory_space=pltpu.VMEM)
    out, sums = pl.pallas_call(
        store,
        out_shape=(jax.ShapeDtypeStruct(out.shape, out.dtype), jax.ShapeDtypeStruct(sums.shape, sums.dtype)),
        in_specs=[vmem_spec] * 2,
        out_specs=(any_spec, any_spec),
        scratch_shapes=[dma((2,))],
    )(*(pltpu.with_memory_space_constraint(v, pltpu.VMEM) for v in (out, sums)))
    return out, sums.reshape(-1)


def solution(mesh):
    classes = mesh.shape["neu"] // KB
    in_specs = (P("neu", "img"), P("neu", "img"), P(None, "neu", None, None), P(None, "neu", None))
    out_specs = (P("neu", "img"), P(("img", "neu")))
    return jax.shard_map(
        functools.partial(on_device, classes, mesh.shape["img"] % 2 == 0), mesh=mesh, in_specs=in_specs,
        out_specs=out_specs, check_vma=False,
    )
```

```python
import functools

import jax
import jax.numpy as jnp
from jax import lax
from jax.experimental import pallas as pl
from jax.experimental.pallas import tpu as pltpu
from jax.sharding import PartitionSpec as P

KB = 4
IB = 8
OB = 32

bias_value = 0.35
ceiling = 32.0


def quotient(x, n):
    return x >> (n.bit_length() - 1) if n & (n - 1) == 0 else lax.div(x, jnp.int32(n))


def remainder(x, n):
    return x & (n - 1) if n & (n - 1) == 0 else lax.rem(x, jnp.int32(n))


def by_position(q, values):
    return (sum(v << (2 * i) for i, v in enumerate(values)) >> (2 * q)) & 3


def kernel(
    geometry, val_hbm, mask_hbm, wt_hbm, idx_hbm, out_ref, rs_ref,
    val, mask, w_src, i_src, i_out, y0, xin, ya, yb, wt, wd, idx_v, idx_s, tiles, part, parts,
    load_sem, own_sem, w_send, w_recv, n_send, f_recv, i_send, i_recv, s_sem, in_send, in_recv, o_send, o_recv,
    r_send, r_recv, here_sem,
):
    classes, pairs, layers, rows, blocks, lanes = geometry
    group = KB
    last = layers - 1
    shift = [l * (l + 1) // 2 % classes for l in range(layers)]
    me = lax.axis_index("neu")
    q, c = me // classes, me % classes
    run_blocks = rows // IB

    middle = (q == 1) | (q == 2)
    other = by_position(q, [3, 2, 1, 0])
    near = by_position(q, [1, 0, 3, 2])
    far = by_position(q, [2, 3, 0, 1])
    order = [
        by_position(q, [3, 3, 0, 0]), by_position(q, [0, 2, 1, 3]),
        by_position(q, [2, 0, 3, 1]), by_position(q, [1, 1, 2, 2]),
    ]

    def to(z, dc):
        return {"neu": z * classes + (c + dc) % classes}

    def remote(src, dst, send, recv, device_id):
        x = pltpu.make_async_remote_copy(
            src_ref=src, dst_ref=dst, send_sem=send, recv_sem=recv,
            device_id=device_id, device_id_type=pl.DeviceIdType.MESH,
        )
        x.start()

    def wait(ref, sem):
        pltpu.make_async_copy(ref, ref, sem).wait()

    own = [
        pltpu.make_async_copy(wt_hbm, w_src, own_sem.at[0]),
        pltpu.make_async_copy(idx_hbm, i_src, own_sem.at[1]),
    ]
    for a in own:
        a.start()
    for p, t in enumerate(order):
        cols = pl.ds(pl.multiple_of(t * lanes, lanes), lanes)
        pltpu.make_async_copy(val_hbm.at[:, cols], val.at[p], load_sem.at[0]).start()
        pltpu.make_async_copy(mask_hbm.at[:, cols], mask.at[p], load_sem.at[1]).start()

    barrier = pltpu.get_barrier_semaphore()
    x_me = lax.axis_index("img")
    half = x_me % 2
    twin = {"img": x_me + 1 - 2 * half}
    share_rows = KB * IB // 2
    w_rows = pl.ds(pl.multiple_of(half * share_rows, share_rows), share_rows) if pairs else pl.ds(0, KB * IB)

    @pl.when(middle)
    def _():
        greet = [to(z, -s) for s in sorted(set(shift)) for z in (far, other)]
        greet += [to(near, dc) for dc in range(classes)]
        greet += [to(q, dc) for dc in range(1, classes)]
        if pairs:
            greet.append(twin)
        for device in greet:
            pl.semaphore_signal(barrier, inc=1, device_id=device, device_id_type=pl.DeviceIdType.MESH)

    def masked(p):
        y0[p] = (val[p].astype(jnp.float32) * mask[p].astype(jnp.float32)).astype(jnp.bfloat16)

    for a in own:
        a.wait()
    b = i_src[...]
    i_out[...] = quotient(b, run_blocks * classes) * run_blocks + remainder(b, run_blocks)

    def send_weights(l, z):
        n = q * layers + l
        if z is q:
            remote(w_src.at[l], wt.at[n], n_send, w_recv.at[q], to(z, shift[l]))
        else:
            remote(w_src.at[l, w_rows], wt.at[n, w_rows], w_send, w_recv.at[q], to(z, shift[l]))

    def send_indices(l, z):
        remote(i_out.at[l], idx_v.at[q * layers + l], i_send, i_recv, to(z, shift[l]))

    def send_input(p, chunk, z):
        remote(y0.at[p], xin.at[chunk, q], in_send, in_recv.at[chunk], to(z, 0))

    unknown = [dc for dc in range(classes) if dc not in shift]

    def own_share(total):
        row = total
        share = lanes // classes
        mine = jnp.zeros((1, share), jnp.float32)
        for j in range(classes):
            mine = jnp.where(c == j, row[:, j * share:(j + 1) * share], mine)
        rs_ref[...] = mine

    @pl.when(jnp.logical_not(middle))
    def _():
        pl.semaphore_wait(barrier, classes + len(set(shift)))
        for z in (far, near):
            for l in range(layers):
                send_weights(l, z)
        for z in (far, near):
            for l in range(layers):
                send_indices(l, z)
        for dc in unknown:
            pl.semaphore_signal(here_sem, inc=1, device_id=to(near, dc), device_id_type=pl.DeviceIdType.MESH)
        wait(val, load_sem.at[0])
        wait(mask, load_sem.at[1])
        wait(wt.at[pl.ds(0, 2 * layers), w_rows], w_send)
        for p in range(group):
            masked(p)
            send_input(p, p // 2, (far, near)[p % 2])
        wait(idx_v.at[pl.ds(0, 2 * layers)], i_send)
        wait(y0, in_send)
        wait(parts.at[pl.ds(0, classes)], r_recv.at[0])
        own_share(sum(parts[dc] for dc in range(classes)))
        wait(out_ref, o_recv)

    @pl.when(middle)
    def _():
        pl.semaphore_wait(barrier, classes - 1 + len(set(shift)) + (1 if pairs else 0))
        for l in range(layers):
            send_weights(l, other)
        for l in range(layers):
            if shift[l]:
                send_weights(l, q)
            else:
                wt[q * layers + l] = w_src[l]
                idx_v[q * layers + l] = i_out[l]
        for l in range(layers):
            send_indices(l, other)
            if shift[l]:
                send_indices(l, q)
        wait(val, load_sem.at[0])
        wait(mask, load_sem.at[1])
        wait(wt.at[pl.ds(0, layers), w_rows], w_send)
        masked(0)
        send_input(0, 0, other)
        masked(1)
        masked(2)
        masked(3)

        local = sum(1 for s in shift if s == 0)
        per = min(4, blocks)
        width = per * OB
        m_of = lax.broadcasted_iota(jnp.int32, (width, width), 0) // (KB * IB)
        n_of = lax.broadcasted_iota(jnp.int32, (width, width), 1) // OB

        def pieces_of(z):
            if z is q:
                return wt.at[pl.ds(z * layers + local, layers - local)]
            return wt.at[pl.ds(z * layers, layers), w_rows]

        def pass_on(z):
            here = pieces_of(z)
            wait(here, w_recv.at[z])
            if pairs and z is not q:
                remote(here, here, w_send, f_recv.at[z], twin)

        def prepare(z, take=True):
            if pairs and z is not q and take:
                wait(pieces_of(z), f_recv.at[z])
            for l in range(layers):
                for g in range(blocks // per):
                    w = wt[z * layers + l, :, g * width:(g + 1) * width].astype(jnp.float32)
                    wide = jnp.where(m_of == n_of, jnp.concatenate([w] * per, axis=0), 0.0)
                    wd[l, z, g] = wide.T.astype(jnp.bfloat16)

        def advance(l, src, t):
            out = []
            for g in range(blocks // per):
                pieces = [src[idx_s[t * layers + l, k, j]] for j in range(g * per, (g + 1) * per) for k in range(KB)]
                picked = jnp.concatenate(pieces, axis=0).astype(jnp.bfloat16)
                summed = jnp.dot(wd[l, t, g], picked, preferred_element_type=jnp.float32)
                clamped = jnp.minimum(jnp.maximum(summed - bias_value, 0.0), ceiling)
                out.append(clamped.astype(jnp.bfloat16))
            return out

        pass_on(other)
        pass_on(near)
        send_input(1, 1, other)
        pass_on(far)
        pass_on(q)
        wait(idx_v.at[pl.ds(0, group * layers - local)], i_recv)
        index_copy = pltpu.make_async_copy(idx_v, idx_s, s_sem)
        index_copy.start()
        prepare(q)
        prepare(other)
        prepare(near)
        index_copy.wait()
        if pairs:
            wait(pieces_of(far), f_recv.at[far])
        pl.semaphore_wait(here_sem, len(unknown))

        for chunk in range(2):
            own_rows = y0[2 + chunk].astype(jnp.float32)
            ya[pl.ds(q * run_blocks, run_blocks)] = own_rows.reshape(run_blocks, IB, lanes)
            wait(xin.at[chunk, pl.ds(0, group - 1)], in_recv.at[chunk])
            if chunk == 0:
                prepare(far, False)
            for z in (other, near, far):
                ya[pl.ds(z * run_blocks, run_blocks)] = xin[chunk, z].astype(jnp.float32).reshape(run_blocks, IB, lanes)

            src, dst = ya, yb
            for l in range(last):
                for t in range(group):
                    for g, y in enumerate(advance(l, src, t)):
                        first = t * run_blocks + g * width // IB
                        dst[first:first + width // IB] = y.astype(jnp.float32).reshape(width // IB, IB, lanes)
                src, dst = dst, src

            tile = near if chunk == 0 else q
            cols = pl.ds(pl.multiple_of(tile * lanes, lanes), lanes)
            targets = (near, far, other, q)
            total = jnp.zeros((8, lanes), jnp.float32)

            def send_tile(d):
                remote(tiles.at[chunk, d], out_ref.at[:, cols], o_send, o_recv, to(targets[d], -shift[last]))

            ready = None
            for d in range(group + 1):
                fresh = advance(last, src, targets[d]) if d < group else None
                if ready is not None:
                    for g, y in enumerate(ready):
                        tiles[chunk, d - 1, g * width:(g + 1) * width, :] = y
                        total = total + jnp.sum(y.astype(jnp.float32).reshape(width // 8, 8, lanes), axis=0)
                    if chunk == 0:
                        send_tile(d - 1)
                ready = fresh
            part[chunk] = jnp.sum(total, axis=0, keepdims=True)
            for dc in range(chunk, classes):
                where = to(q, dc) if chunk else to(near, dc)
                remote(part.at[chunk], parts.at[chunk * classes + dc], r_send, r_recv.at[chunk], where)
            if chunk:
                for d in range(group):
                    send_tile(d)

        wait(parts.at[pl.ds(classes + 1, classes - 1)], r_recv.at[1])
        own_share(part[1] + sum(parts[classes + dc] for dc in range(1, classes)))
        if pairs:
            wait(wt.at[pl.ds(0, 3 * layers), w_rows], w_send)
        wait(wt.at[pl.ds(0, layers - local)], n_send)
        wait(idx_v.at[pl.ds(0, 2 * layers - local)], i_send)
        wait(y0.at[pl.ds(0, 2)], in_send)
        wait(tiles, o_send)
        wait(parts.at[pl.ds(0, 2 * classes - 1)], r_send)
        wait(out_ref, o_recv)


def store(out_ref, rs_ref, out_hbm, rs_hbm, sems):
    a = pltpu.make_async_copy(out_ref, out_hbm, sems.at[0])
    step = out_ref.shape[0] // 4
    b = pltpu.make_async_copy(rs_ref, rs_hbm, sems.at[1])
    b.start()
    for n in range(4):
        rows = pl.ds(n * step, step)
        pltpu.make_async_copy(out_ref.at[rows], out_hbm.at[rows], sems.at[0]).start()
    a.wait()
    b.wait()


def on_device(classes, pairs, image_values, image_mask, weights, block_index):
    layers, rows = weights.shape[:2]
    blocks = block_index.shape[1]
    columns = image_values.shape[1]
    group = KB
    lanes = columns // group
    wt = jnp.transpose(weights, (0, 2, 3, 1)).reshape(layers, KB * IB, rows)
    idx = jnp.transpose(block_index, (0, 2, 1))
    per = min(4, blocks)
    bf16, f32, i32 = jnp.bfloat16, jnp.float32, jnp.int32
    V, S = pltpu.VMEM, pltpu.SMEM
    dma = pltpu.SemaphoreType.DMA
    any_spec = pl.BlockSpec(memory_space=pl.ANY)
    operands = [pltpu.with_memory_space_constraint(v, pltpu.HBM) for v in (image_values, image_mask, wt, idx)]
    out, sums = pl.pallas_call(
        functools.partial(kernel, (classes, pairs, layers, rows, blocks, lanes)),
        out_shape=(
            jax.ShapeDtypeStruct((rows, columns), bf16),
            jax.ShapeDtypeStruct((1, lanes // classes), f32),
        ),
        in_specs=[any_spec] * 4,
        out_specs=(pl.BlockSpec(memory_space=pltpu.VMEM), pl.BlockSpec(memory_space=pltpu.VMEM)),
        scratch_shapes=[
            V((group, rows, lanes), bf16),
            V((group, rows, lanes), i32),
            V((layers, KB * IB, rows), bf16),
            V((layers, KB, blocks), i32),
            V((layers, KB, blocks), i32),
            V((group, rows, lanes), bf16),
            V((2, group, rows, lanes), bf16),
            V((group * rows // IB, IB, lanes), f32),
            V((group * rows // IB, IB, lanes), f32),
            V((group * layers, KB * IB, rows), bf16),
            V((layers, group, blocks // per, per * OB, per * KB * IB), bf16),
            V((group * layers, KB, blocks), i32),
            S((group * layers, KB, blocks), i32),
            V((2, group, rows, lanes), bf16),
            V((2, 1, lanes), f32),
            V((2 * classes, 1, lanes), f32),
            dma((2,)), dma((2,)),
            dma(()), dma((group,)), dma(()), dma((group,)),
            dma(()), dma(()), dma(()),
            dma(()), dma((2,)),
            dma(()), dma(()),
            dma(()), dma((2,)), pltpu.SemaphoreType.REGULAR,
        ],
        compiler_params=pltpu.CompilerParams(collective_id=0, has_side_effects=True, vmem_limit_bytes=16 * 1024 * 1024),
    )(*operands)
    vmem_spec = pl.BlockSpec(memory_space=pltpu.VMEM)
    out, sums = pl.pallas_call(
        store,
        out_shape=(jax.ShapeDtypeStruct(out.shape, out.dtype), jax.ShapeDtypeStruct(sums.shape, sums.dtype)),
        in_specs=[vmem_spec] * 2,
        out_specs=(any_spec, any_spec),
        scratch_shapes=[dma((2,))],
    )(*(pltpu.with_memory_space_constraint(v, pltpu.VMEM) for v in (out, sums)))
    return out, sums.reshape(-1)


def solution(mesh):
    classes = mesh.shape["neu"] // KB
    in_specs = (P("neu", "img"), P("neu", "img"), P(None, "neu", None, None), P(None, "neu", None))
    out_specs = (P("neu", "img"), P(("img", "neu")))
    return jax.shard_map(
        functools.partial(on_device, classes, mesh.shape["img"] % 2 == 0), mesh=mesh, in_specs=in_specs,
        out_specs=out_specs, check_vma=False,
    )
```
